256 devices in a mesh: img: 16 (over y, x), row: 16 (over z, core).
Axes of the slice: x: 4, y: 4, z: 8, core: 2. Of those that a mesh axis runs over, the one named last changes fastest.
Arguments:
- latent: bfloat16 [1024, 128, 512], P(('img', 'row')), parts along dimension 0, may hold values from -8 to 8
- attn_gain: float32 [512], replicated, may hold values from 0.5 to 1.5
- attn_shift: float32 [512], replicated, may hold values from -3 to 3
- w_query: bfloat16 [512, 512], replicated, may hold values from -2 to 2
- w_key: bfloat16 [512, 512], replicated, may hold values from -2 to 2
- w_value: bfloat16 [512, 512], replicated, may hold values from -0.25 to 0.25
- w_out: bfloat16 [512, 512], replicated, may hold values from -0.25 to 0.25
- conv_gain: float32 [512], replicated, may hold values from 0.5 to 1.5
- conv_shift: float32 [512], replicated, may hold values from -3 to 3
- w_conv: bfloat16 [3, 3, 512, 512], replicated, may hold values from -0.09375 to 0.09375
- conv_bias: float32 [512], replicated, may hold values from -3 to 3
Outputs:
- encoded: bfloat16 [1024, 128, 512], P(('img', 'row')), parts along dimension 0
The draws below stay inside these ranges and needn't reach their ends.
There are 16 independent parts, one for each index of `img`. The reference program is written for one: setup_inputs(seed, part) draws one part's arguments, and reference() takes and returns one part's arrays. A program takes and returns all parts, laid end to end along the dimension named above; an argument that names none is the same for every part. Nothing has to cross between parts.
All inputs are finite; a program needn't handle non-finite values.
Results may differ from the reference program's by a relative error of at most 0.011.
Values may be sent and summed in bfloat16 or wider, within the bound.
A program may use at most 128 MiB of HBM per device.

```python
import jax
import jax.numpy as jnp
from jax import lax

C = 512
GROUPS = 32
W = 128
H = 64


def shared_gauss(key):
    return jnp.clip(jax.random.normal(jax.random.fold_in(key, 7), (C, C), jnp.float32), -3.0, 3.0)


def draw_latent(key, part):
    noise = jax.random.normal(jax.random.fold_in(key, 3), (H, W, C), jnp.float32)
    rows = (jnp.arange(H, dtype=jnp.float32) + 0.5) / H
    phase = jax.random.uniform(jax.random.fold_in(key, 13), (GROUPS,), jnp.float32, -jnp.pi, jnp.pi)
    amplitude = jax.random.uniform(jax.random.fold_in(key, 17), (C,), jnp.float32, 0.8, 1.6)
    wave = jnp.sin(2.0 * jnp.pi * rows[:, None] + phase[None, :])
    offset = jnp.repeat(wave, C // GROUPS, axis=1) * amplitude[None, :]
    result = noise + offset[:, None, :]
    return jnp.clip(result, -8.0, 8.0).astype(jnp.bfloat16)


def draw_w_query(key, part):
    return (shared_gauss(key) * (4.0 / jnp.sqrt(jnp.float32(C)))).astype(jnp.bfloat16)


def draw_w_key(key, part):
    fresh = jnp.clip(jax.random.normal(jax.random.fold_in(key, 11), (C, C), jnp.float32), -3.0, 3.0)
    result = fresh / jnp.sqrt(jnp.float32(C))
    return result.astype(jnp.bfloat16)


def scatter_about(stream_key, extent, scale, most, kind=jnp.bfloat16):
    return jnp.clip(scale * jax.random.normal(stream_key, extent, jnp.float32), -most, most).astype(kind)


def setup_inputs(seed: int = 0, part: int = 0) -> dict:
    key_list = jax.random.split(jax.random.key(seed), 12)
    part_splits = jax.random.split(jax.random.fold_in(key_list[11], part), 12)
    return {
        "latent": draw_latent(jax.random.fold_in(jax.random.fold_in(key_list[11], part), 71), part),
        "attn_gain": jnp.clip(1.0 + 0.1 * jax.random.normal(key_list[1], (C,), jnp.float32), 0.5, 1.5),
        "attn_shift": scatter_about(key_list[2], (C,), 0.5, 3.0, jnp.float32),
        "w_query": draw_w_query(jax.random.fold_in(key_list[11], 71), part),
        "w_key": draw_w_key(jax.random.fold_in(key_list[11], 71), part),
        "w_value": scatter_about(key_list[5], (C, C), C ** -0.5, 0.25),
        "w_out": scatter_about(key_list[6], (C, C), C ** -0.5, 0.25),
        "conv_gain": jnp.clip(1.0 + 0.1 * jax.random.normal(key_list[7], (C,), jnp.float32), 0.5, 1.5),
        "conv_shift": scatter_about(key_list[8], (C,), 0.5, 3.0, jnp.float32),
        "w_conv": scatter_about(key_list[9], (3, 3, C, C), (9 * C) ** -0.5, 0.09375),
        "conv_bias": scatter_about(key_list[10], (C,), 0.5, 3.0, jnp.float32),
    }


epsilon = 1e-06

def group_norm(field, gain, shift):
    grouped = field.astype(jnp.float32).reshape(field.shape[0], GROUPS, C // GROUPS)
    centre = lax.optimization_barrier(jnp.mean(grouped, axis=(0, 2)))
    offset = grouped - centre[None, :, None]
    spread = lax.optimization_barrier(jnp.mean(offset * offset, axis=(0, 2)))
    normed = offset * lax.rsqrt(spread + epsilon)[None, :, None]
    return normed.reshape(field.shape) * gain + shift

def reference(latent, attn_gain, attn_shift, w_query, w_key, w_value, w_out, conv_gain, conv_shift, w_conv, conv_bias):
    positions = latent.reshape(H * W, C)
    normed = group_norm(positions, attn_gain, attn_shift).astype(jnp.bfloat16)
    queries = jnp.dot(normed, w_query, preferred_element_type=jnp.float32).astype(jnp.bfloat16)
    key_rows = jnp.dot(normed, w_key, preferred_element_type=jnp.float32).astype(jnp.bfloat16)
    values = jnp.dot(normed, w_value, preferred_element_type=jnp.float32).astype(jnp.bfloat16)
    scaling = 1.0 / jnp.sqrt(jnp.float32(C))
    scores = jnp.einsum('qc,kc->qk', queries.astype(jnp.float32), key_rows.astype(jnp.float32)) * scaling
    rowmax = lax.optimization_barrier(jnp.max(scores, axis=1))
    expo = jnp.exp(scores - rowmax[:, None])
    denominator = lax.optimization_barrier(jnp.sum(expo, axis=1))
    probs = expo.astype(jnp.bfloat16)
    attended = (jnp.dot(probs, values, preferred_element_type=jnp.float32) / denominator[:, None]).astype(jnp.bfloat16)
    hidden = (positions.astype(jnp.float32) + jnp.dot(attended, w_out, preferred_element_type=jnp.float32)).astype(jnp.bfloat16)
    activated = jax.nn.silu(group_norm(hidden, conv_gain, conv_shift)).astype(jnp.bfloat16).reshape(H, W, C)
    padded = jnp.pad(activated, ((1, 1), (1, 1), (0, 0)))
    convolved = jnp.zeros((H * W, C), jnp.float32)
    for row_tap in range(3):
        for col_tap in range(3):
            window = padded[row_tap:row_tap + H, col_tap:col_tap + W].reshape(H * W, C)
            convolved = convolved + jnp.dot(window, w_conv[row_tap, col_tap], preferred_element_type=jnp.float32)
    encoded = hidden.astype(jnp.float32) + (convolved + conv_bias)
    return encoded.astype(jnp.bfloat16).reshape(H, W, C)
```

```python
import jax
import jax.numpy as jnp
from jax import lax
from jax.experimental import pallas as pl
from jax.experimental.pallas import tpu as pltpu
from jax.sharding import PartitionSpec as P

C = 512
W = 128
ROWS = 4
N = ROWS * W
CH = 128
GROUP = 16
DEV = 16
ZN = 8
SENDS = 14
EPS = 1e-06
F32 = jnp.float32
BF16 = jnp.bfloat16
LOG2E = 1.4426950408889634

NT = (((1,), (1,)), ((), ()))


def dot(a, b, dims=(((1,), (0,)), ((), ()))):
    return lax.dot_general(a, b, dims, preferred_element_type=F32)


def group_total(v):
    lane = lax.broadcasted_iota(jnp.int32, v.shape, v.ndim - 1)
    step = 1
    while step < GROUP:
        up = pltpu.roll(v, 128 - step, v.ndim - 1)
        down = pltpu.roll(v, step, v.ndim - 1)
        v = v + jnp.where((lane // step) % 2 == 0, up, down)
        step *= 2
    return v


def as_line(v):
    return jnp.concatenate([v[i : i + 1, :] for i in range(4)], axis=1)


def local_moments(read, buf):
    total = jnp.zeros((8, C), F32)
    for i in range(4):
        part = read(i).astype(F32).reshape(CH // 8, 8, C)
        total = total + jnp.sum(part, axis=0)
    mean = jnp.sum(total, axis=0, keepdims=True) * (1.0 / N)
    dev = jnp.zeros((8, C), F32)
    for i in range(4):
        off = read(i).astype(F32).reshape(CH // 8, 8, C) - mean[None]
        dev = dev + jnp.sum(off * off, axis=0)
    dev = jnp.sum(dev, axis=0, keepdims=True)
    for i in range(4):
        buf[i : i + 1, :] = mean[:, 128 * i : 128 * i + 128]
        buf[4 + i : 5 + i, :] = dev[:, 128 * i : 128 * i + 128]


def combined(stats, own):
    means = [own[0:4, :]]
    devs = [own[4:8, :]]
    for i in range(DEV - 1):
        means.append(stats[i, 0:4, :])
        devs.append(stats[i, 4:8, :])
    centre = group_total(sum(means[1:], means[0])) * (1.0 / (DEV * GROUP))
    spread = jnp.zeros((4, 128), F32)
    for m, d in zip(means, devs):
        off = m - centre
        spread = spread + (d + float(N) * (off * off))
    spread = group_total(spread) * (1.0 / (DEV * GROUP * N))
    return as_line(centre), as_line(lax.rsqrt(spread + EPS))


def kernel(
    x_hbm, ag_h, as_h, wq_h, wk_h, wv_h, wo_h, cg_h, cs_h, wc_h, cb_h,
    out_ref,
    kv, wq, wk, wv, wo, wc, vecs, q_s, acc, m_s, l_s, hid, halo, lhs, mine, stat_a, stat_b,
    load_sem, w_sem, wc_sem, v_sem,
    ring_send, ring_recv, sib_send, sib_recv, own_send, own_recv,
    sa_send, sa_recv, sb_send, sb_recv, h_send, h_recv,
):
    me = lax.axis_index("row")
    z = me // 2
    core = me % 2
    right = ((z + 1) % ZN) * 2 + core
    left = ((z + ZN - 1) % ZN) * 2 + core
    sib = z * 2 + (1 - core)

    loads = [
        pltpu.make_async_copy(x_hbm.at[pl.ds(CH * i, CH)], kv.at[me, i], load_sem.at[i])
        for i in range(4)
    ]
    for c in loads:
        c.start()

    barrier = pltpu.get_barrier_semaphore()
    for d in range(1, DEV):
        pl.semaphore_signal(barrier, inc=1, device_id={"row": (me + d) % DEV})

    small = [
        pltpu.make_async_copy(src, vecs.at[i], v_sem.at[i])
        for i, src in enumerate((ag_h, as_h, cg_h, cs_h, cb_h))
    ]
    for c in small:
        c.start()
    weights = [
        pltpu.make_async_copy(src, dst, w_sem.at[i])
        for i, (src, dst) in enumerate(((wq_h, wq), (wk_h, wk), (wv_h, wv), (wo_h, wo)))
    ]
    for c in weights:
        c.start()
    taps = [
        pltpu.make_async_copy(
            wc_h.at[dy, dx], wc.at[dx, pl.ds(C * dy, C)], wc_sem.at[3 * dy + dx]
        )
        for dy in range(3)
        for dx in range(3)
    ]
    for c in taps:
        c.start()

    def ring(way, blk, chunk, j):
        return pltpu.make_async_remote_copy(
            src_ref=kv.at[blk, chunk],
            dst_ref=kv.at[blk, chunk],
            send_sem=ring_send.at[way, j],
            recv_sem=ring_recv.at[way, j],
            device_id={"row": right if way == 0 else left},
        )

    def to_sib(blk, chunk, sends, recvs):
        return pltpu.make_async_remote_copy(
            src_ref=kv.at[blk, chunk],
            dst_ref=kv.at[blk, chunk],
            send_sem=sends,
            recv_sem=recvs,
            device_id={"row": sib},
        )

    def stat_copy(d, dst, sends, recvs):
        return pltpu.make_async_remote_copy(
            src_ref=mine,
            dst_ref=dst.at[d - 1],
            send_sem=sends.at[d - 1],
            recv_sem=recvs.at[d - 1],
            device_id={"row": (me + d) % DEV},
        )

    pl.semaphore_wait(barrier, DEV - 1)

    order = ((0, 2), (1, 3), (2, 0), (3, 1))
    loads[0].wait()
    ring(0, me, 0, 0).start()
    loads[2].wait()
    ring(1, me, 2, 0).start()
    loads[1].wait()
    loads[3].wait()

    local_moments(lambda i: kv[me, i], mine)
    for d in range(1, DEV):
        stat_copy(d, stat_a, sa_send, sa_recv).start()
    for j in range(1, 4):
        ring(0, me, order[j][0], j).start()
        ring(1, me, order[j][1], j).start()
    for i in range(4):
        to_sib(me, i, own_send.at[i], own_recv.at[i]).start()

    m_s[...] = jnp.full_like(m_s, -1e30)
    l_s[...] = jnp.zeros_like(l_s)
    acc[...] = jnp.zeros_like(acc)

    for c in weights:
        c.wait()
    wv[...] = dot(wv[...], wo[...]).astype(BF16)

    def came(i):
        chunk = i % 4
        far = i // 4 + 1
        blk_r = ((z + ZN - far) % ZN) * 2 + core
        blk_l = ((z + far) % ZN) * 2 + core
        return blk_r, chunk, blk_l, (chunk + 2) % 4

    def comm(i):
        blk_r, cr, blk_l, cl = came(i)
        ring(0, blk_r, cr, i).wait_recv()
        ring(1, blk_l, cl, i).wait_recv()

        @pl.when(i < SENDS - 4)
        def _():
            ring(0, blk_r, cr, i + 4).start()
            ring(1, blk_l, cl, i + 4).start()

        to_sib(blk_r, cr, sib_send.at[0, i], sib_recv.at[0, i]).start()
        to_sib(blk_l, cl, sib_send.at[1, i], sib_recv.at[1, i]).start()

    def attend(blk_a, ca, blk_b, cb):
        keys = jnp.concatenate([kv[blk_a, ca], kv[blk_b, cb]], axis=0)
        for t in range(2):
            rows = pl.ds(256 * t, 256)
            s = dot(q_s[rows, :], keys, NT)
            m_old = m_s[rows, :]
            m_new = jnp.maximum(m_old, jnp.max(s, axis=1, keepdims=True))
            alpha = jnp.exp2(m_old - m_new)
            p0 = jnp.exp2(s[:, :128] - m_new).astype(BF16)
            p1 = jnp.exp2(s[:, 128:] - m_new).astype(BF16)
            l_s[rows, :] = l_s[rows, :] * alpha + (p0.astype(F32) + p1.astype(F32))
            m_s[rows, :] = m_new
            pv = dot(jnp.concatenate([p0, p1], axis=1), keys)
            acc[rows, :] = acc[rows, :] * jnp.concatenate([alpha] * 4, axis=1) + pv

    comm(0)

    for c in small:
        c.wait()
    for d in range(1, DEV):
        stat_copy(d, stat_a, sa_send, sa_recv).wait()
    mean, rs = combined(stat_a, mine)
    scale = rs * vecs[0]
    shift = vecs[1]
    for i in range(4):
        normed = ((kv[me, i].astype(F32) - mean) * scale + shift).astype(BF16)
        query = dot(normed, wq[...]).astype(BF16)
        folded = dot(query, wk[...], NT) * (scale * (LOG2E / C**0.5))
        q_s[CH * i : CH * i + CH, :] = folded.astype(BF16)

    for i in range(4):
        to_sib(me, i, own_send.at[i], own_recv.at[i]).wait_recv()

    def first(k, carry):
        blk = jnp.where(k < 2, me, sib)
        attend(blk, 2 * (k % 2), blk, 2 * (k % 2) + 1)
        return carry

    lax.fori_loop(0, 4, first, 0)

    def other(i):
        blk_r, cr, blk_l, cl = came(i)
        return blk_r + 1 - 2 * core, cr, blk_l + 1 - 2 * core, cl

    def sib_wait(i):
        blk_r, cr, blk_l, cl = other(i)
        to_sib(blk_r, cr, sib_send.at[0, i], sib_recv.at[0, i]).wait_recv()
        to_sib(blk_l, cl, sib_send.at[1, i], sib_recv.at[1, i]).wait_recv()

    def body(i, carry):
        @pl.when(i > 0)
        def _():
            comm(i)
            sib_wait(i - 1)
            attend(*other(i - 1))

        attend(*came(i))
        return carry

    lax.fori_loop(0, SENDS, body, 0)
    sib_wait(SENDS - 1)
    attend(*other(SENDS - 1))

    for t in range(4):
        rows = pl.ds(CH * t, CH)
        inv = 1.0 / jnp.sum(l_s[rows, :], axis=1, keepdims=True)
        att = ((acc[rows, :] * inv - mean) * scale + shift).astype(BF16)
        hid[t] = (kv[me, t].astype(F32) + dot(att, wv[...])).astype(BF16)

    def halo_copy(k, row, peer):
        return pltpu.make_async_remote_copy(
            src_ref=hid.at[row],
            dst_ref=halo.at[k],
            send_sem=h_send.at[k],
            recv_sem=h_recv.at[k],
            device_id={"row": peer},
        )

    down = halo_copy(0, ROWS - 1, (me + 1) % DEV)
    up = halo_copy(1, 0, (me + DEV - 1) % DEV)
    down.start()
    up.start()
    local_moments(lambda i: hid[i], mine)
    for d in range(1, DEV):
        stat_copy(d, stat_b, sb_send, sb_recv).start()
    for c in taps:
        c.wait()
    down.wait()
    up.wait()
    for d in range(1, DEV):
        stat_copy(d, stat_b, sb_send, sb_recv).wait()
    mean2, rs2 = combined(stat_b, mine)
    scale2 = rs2 * vecs[2] * 0.5
    shift2 = vecs[3] * 0.5

    for j in range(ROWS + 2):
        src = halo[0] if j == 0 else halo[1] if j == ROWS + 1 else hid[j - 1]
        half = (src.astype(F32) - mean2) * scale2 + shift2
        act = half + half * jnp.tanh(half)
        if j == 0:
            act = jnp.where(me == 0, 0.0, act)
        if j == ROWS + 1:
            act = jnp.where(me == DEV - 1, 0.0, act)
        act = act.astype(BF16)
        for dy in range(3):
            i = j - dy
            if 0 <= i < ROWS:
                lhs[CH * i : CH * i + CH, C * dy : C * dy + C] = act

    col = lax.broadcasted_iota(jnp.int32, (N, 256), 0) % W
    for n in range(2):
        cols = slice(256 * n, 256 * n + 256)
        t0 = dot(lhs[...], wc[0, :, cols])
        t1 = dot(lhs[...], wc[1, :, cols])
        t2 = dot(lhs[...], wc[2, :, cols])
        total = t1 + jnp.where(col == 0, 0.0, pltpu.roll(t0, 1, 0))
        total = total + jnp.where(col == W - 1, 0.0, pltpu.roll(t2, N - 1, 0))
        base = jnp.concatenate([hid[i, :, cols] for i in range(4)], axis=0).astype(F32)
        out_ref[:, cols] = (base + (total + vecs[4, :, cols])).astype(BF16)

    def drain(i, carry):
        blk_r, cr, blk_l, cl = came(i)
        ring(0, blk_r, cr, i).wait_send()
        ring(1, blk_l, cl, i).wait_send()
        to_sib(blk_r, cr, sib_send.at[0, i], sib_recv.at[0, i]).wait_send()
        to_sib(blk_l, cl, sib_send.at[1, i], sib_recv.at[1, i]).wait_send()
        return carry

    lax.fori_loop(0, SENDS, drain, 0)
    for i in range(4):
        to_sib(me, i, own_send.at[i], own_recv.at[i]).wait_send()


def local(
    latent, attn_gain, attn_shift, w_query, w_key, w_value, w_out,
    conv_gain, conv_shift, w_conv, conv_bias,
):
    line = lambda v: v.reshape(1, C)
    dma = pltpu.SemaphoreType.DMA
    out = pl.pallas_call(
        kernel,
        out_shape=jax.ShapeDtypeStruct((N, C), BF16),
        in_specs=[pl.BlockSpec(memory_space=pl.ANY)] * 11,
        out_specs=pl.BlockSpec(memory_space=pltpu.VMEM),
        scratch_shapes=[
            pltpu.VMEM((DEV, 4, CH, C), BF16),
            pltpu.VMEM((C, C), BF16),
            pltpu.VMEM((C, C), BF16),
            pltpu.VMEM((C, C), BF16),
            pltpu.VMEM((C, C), BF16),
            pltpu.VMEM((3, 3 * C, C), BF16),
            pltpu.VMEM((5, 1, C), F32),
            pltpu.VMEM((N, C), BF16),
            pltpu.VMEM((N, C), F32),
            pltpu.VMEM((N, 128), F32),
            pltpu.VMEM((N, 128), F32),
            pltpu.VMEM((ROWS, W, C), BF16),
            pltpu.VMEM((2, W, C), BF16),
            pltpu.VMEM((N, 3 * C), BF16),
            pltpu.VMEM((8, 128), F32),
            pltpu.VMEM((DEV - 1, 8, 128), F32),
            pltpu.VMEM((DEV - 1, 8, 128), F32),
            dma((4,)),
            dma((4,)),
            dma((9,)),
            dma((5,)),
            dma((2, SENDS)),
            dma((2, SENDS)),
            dma((2, SENDS)),
            dma((2, SENDS)),
            dma((4,)),
            dma((4,)),
            dma((DEV - 1,)),
            dma((DEV - 1,)),
            dma((DEV - 1,)),
            dma((DEV - 1,)),
            dma((2,)),
            dma((2,)),
        ],
        compiler_params=pltpu.CompilerParams(
            collective_id=0, has_side_effects=True, vmem_limit_bytes=60 * 1024 * 1024
        ),
    )(
        latent.reshape(N, C), line(attn_gain), line(attn_shift), w_query, w_key, w_value, w_out,
        line(conv_gain), line(conv_shift), w_conv, line(conv_bias),
    )
    return out.reshape(ROWS, W, C)


def solution(mesh):
    part = P(("img", "row"), None, None)
    return jax.shard_map(
        local, mesh=mesh, in_specs=(part,) + (P(),) * 10, out_specs=part, check_vma=False
    )
```

```python
import jax
import jax.numpy as jnp
from jax import lax
from jax.experimental import pallas as pl
from jax.experimental.pallas import tpu as pltpu
from jax.sharding import PartitionSpec as P

C = 512
W = 128
ROWS = 4
N = ROWS * W
CH = 128
GROUP = 16
DEV = 16
ZN = 8
SENDS = 14
TILE = 256
EPS = 1e-06
F32 = jnp.float32
BF16 = jnp.bfloat16
LOG2E = 1.4426950408889634

NT = (((1,), (1,)), ((), ()))


def dot(a, b, dims=(((1,), (0,)), ((), ()))):
    return lax.dot_general(a, b, dims, preferred_element_type=F32)


def as_line(v):
    return jnp.concatenate([v[i : i + 1, :] for i in range(4)], axis=1)


def put_moments(first, total, square, buf):
    total = jnp.sum(total, axis=0, keepdims=True)
    square = jnp.sum(square, axis=0, keepdims=True)
    off = total * (1.0 / N)
    dev = jnp.maximum(square - total * off, 0.0)
    mean = first + off
    for i in range(4):
        buf[i : i + 1, :] = mean[:, 128 * i : 128 * i + 128]
        buf[4 + i : 5 + i, :] = dev[:, 128 * i : 128 * i + 128]


def sums_about(first, block):
    off = (block - first).reshape(block.shape[0] // 8, 8, C)
    return jnp.sum(off, axis=0), jnp.sum(off * off, axis=0)


def combined(stats, own):
    means = [own[0:4, :]] + [stats[i, 0:4, :] for i in range(DEV - 1)]
    devs = [own[4:8, :]] + [stats[i, 4:8, :] for i in range(DEV - 1)]
    centre = sum(means[1:], means[0]) * (1.0 / DEV)
    spread = jnp.zeros((4, 128), F32)
    for m, d in zip(means, devs):
        off = m - centre
        spread = spread + (d + float(N) * (off * off))
    lane = lax.broadcasted_iota(jnp.int32, (4, 128), 1)
    count = float(N * DEV)
    step = 1
    while step < GROUP:
        low = (lane // step) % 2 == 0
        both = []
        for v in (centre, spread):
            both.append(jnp.where(low, pltpu.roll(v, 128 - step, 1), pltpu.roll(v, step, 1)))
        gap = both[0] - centre
        spread = spread + both[1] + (0.5 * count) * (gap * gap)
        centre = 0.5 * (centre + both[0])
        step *= 2
        count *= 2.0
    return as_line(centre), as_line(lax.rsqrt(spread * (1.0 / count) + EPS))


def kernel(
    x_hbm, ag_h, as_h, wq_h, wk_h, wv_h, wo_h, cg_h, cs_h, wc_h,
    hid, edges, coef, wc,
    kv, wq, wk, wv, wo, vecs, q_s, acc, m_s, l_s, halo, mine, stat_a, stat_b,
    load_sem, w_sem, wc_sem, v_sem,
    ring_send, ring_recv, sib_send, sib_recv, own_send, own_recv,
    sa_send, sa_recv, sb_send, sb_recv, h_send, h_recv, known,
):
    me = lax.axis_index("row")
    z = me // 2
    core = me % 2
    right = ((z + 1) % ZN) * 2 + core
    left = ((z + ZN - 1) % ZN) * 2 + core
    sib = z * 2 + (1 - core)

    loads = [
        pltpu.make_async_copy(x_hbm.at[pl.ds(CH * i, CH)], kv.at[me, i], load_sem.at[i])
        for i in range(4)
    ]
    for c in loads:
        c.start()

    barrier = pltpu.get_barrier_semaphore()
    for peer in (left, right, sib):
        pl.semaphore_signal(barrier, inc=1, device_id={"row": peer})

    small = [
        pltpu.make_async_copy(src, vecs.at[i], v_sem.at[i])
        for i, src in enumerate((ag_h, as_h, cg_h, cs_h))
    ]
    for c in small:
        c.start()
    weights = [
        pltpu.make_async_copy(src, dst, w_sem.at[i])
        for i, (src, dst) in enumerate(((wq_h, wq), (wk_h, wk), (wv_h, wv), (wo_h, wo)))
    ]
    for c in weights:
        c.start()
    taps = [
        pltpu.make_async_copy(
            wc_h.at[dy, dx], wc.at[dx, pl.ds(C * dy, C)], wc_sem.at[3 * dy + dx]
        )
        for dy in range(3)
        for dx in range(3)
    ]
    for c in taps:
        c.start()

    def ring(way, blk, chunk, j):
        return pltpu.make_async_remote_copy(
            src_ref=kv.at[blk, chunk],
            dst_ref=kv.at[blk, chunk],
            send_sem=ring_send.at[way, j],
            recv_sem=ring_recv.at[way, j],
            device_id={"row": right if way == 0 else left},
        )

    def to_sib(blk, chunk, sends, recvs):
        return pltpu.make_async_remote_copy(
            src_ref=kv.at[blk, chunk],
            dst_ref=kv.at[blk, chunk],
            send_sem=sends,
            recv_sem=recvs,
            device_id={"row": sib},
        )

    def stat_copy(d, dst, sends, recvs):
        return pltpu.make_async_remote_copy(
            src_ref=mine,
            dst_ref=dst.at[d - 1],
            send_sem=sends.at[d - 1],
            recv_sem=recvs.at[d - 1],
            device_id={"row": (me + d) % DEV},
        )

    pl.semaphore_wait(barrier, 3)

    order = ((0, 2), (1, 3), (2, 0), (3, 1))
    loads[0].wait()
    ring(0, me, 0, 0).start()
    loads[2].wait()
    ring(1, me, 2, 0).start()
    loads[1].wait()
    loads[3].wait()
    ring(0, me, 1, 1).start()
    ring(1, me, 3, 1).start()

    far_right = ((z + 2) % ZN) * 2 + core
    far_left = ((z + ZN - 2) % ZN) * 2 + core
    for k, peers in enumerate(((left, right, sib), (far_left, far_right), (sib,))):
        for peer in peers:
            pl.semaphore_signal(known.at[k], inc=1, device_id={"row": peer})
        if k == 0:
            base = kv[me, 0, 0:1, :].astype(F32)
            sums = [sums_about(base, kv[me, i].astype(F32)) for i in range(4)]
            put_moments(base, sum(a for a, _ in sums), sum(b for _, b in sums), mine)
        pl.semaphore_wait(known.at[k], len(peers))

    for d in range(1, DEV):
        stat_copy(d, stat_a, sa_send, sa_recv).start()
    for j in range(2, 4):
        ring(0, me, order[j][0], j).start()
        ring(1, me, order[j][1], j).start()
    for i in range(4):
        to_sib(me, i, own_send.at[i], own_recv.at[i]).start()

    m_s[...] = jnp.full_like(m_s, -1e30)
    l_s[...] = jnp.zeros_like(l_s)
    acc[...] = jnp.zeros_like(acc)

    for c in weights:
        c.wait()
    wv[...] = dot(wv[...], wo[...]).astype(BF16)

    def came(i):
        chunk = i % 4
        far = i // 4 + 1
        blk_r = ((z + ZN - far) % ZN) * 2 + core
        blk_l = ((z + far) % ZN) * 2 + core
        return blk_r, chunk, blk_l, (chunk + 2) % 4

    def comm(i):
        blk_r, cr, blk_l, cl = came(i)
        ring(0, blk_r, cr, i).wait_recv()
        ring(1, blk_l, cl, i).wait_recv()

        @pl.when(i < SENDS - 4)
        def _():
            ring(0, blk_r, cr, i + 4).start()
            ring(1, blk_l, cl, i + 4).start()

        to_sib(blk_r, cr, sib_send.at[0, i], sib_recv.at[0, i]).start()
        to_sib(blk_l, cl, sib_send.at[1, i], sib_recv.at[1, i]).start()

    def attend(*chunks):
        keys = jnp.concatenate([kv[blk, chunk] for blk, chunk in chunks], axis=0)
        spans = range(0, CH * len(chunks), 128)

        def weigh(rows, s):
            m_old = m_s[rows, :]
            m_new = jnp.maximum(m_old, jnp.max(s, axis=1, keepdims=True))
            alpha = jnp.exp2(m_old - m_new)
            p = [jnp.exp2(s[:, k : k + 128] - m_new).astype(BF16) for k in spans]
            l_s[rows, :] = l_s[rows, :] * alpha + sum(v.astype(F32) for v in p)
            m_s[rows, :] = m_new
            return jnp.concatenate([alpha] * 4, axis=1), jnp.concatenate(p, axis=1)

        tiles = [pl.ds(TILE * t, TILE) for t in range(N // TILE)]
        s = dot(q_s[tiles[0], :], keys, NT)
        for t, rows in enumerate(tiles):
            ahead = dot(q_s[tiles[t + 1], :], keys, NT) if t + 1 < len(tiles) else None
            alpha, p = weigh(rows, s)
            acc[rows, :] = acc[rows, :] * alpha + dot(p, keys)
            s = ahead

    comm(0)

    for c in small:
        c.wait()
    for d in range(1, DEV):
        stat_copy(d, stat_a, sa_send, sa_recv).wait()
    mean, rs = combined(stat_a, mine)
    scale = rs * vecs[0]
    shift = vecs[1]
    for i in range(4):
        normed = ((kv[me, i].astype(F32) - mean) * scale + shift).astype(BF16)
        query = dot(normed, wq[...]).astype(BF16)
        folded = dot(query, wk[...], NT) * (scale * (LOG2E / C**0.5))
        q_s[CH * i : CH * i + CH, :] = folded.astype(BF16)

    for i in range(4):
        to_sib(me, i, own_send.at[i], own_recv.at[i]).wait_recv()

    def first(k, carry):
        blk = jnp.where(k < 1, me, sib)
        attend((blk, 0), (blk, 1), (blk, 2), (blk, 3))
        return carry

    lax.fori_loop(0, 2, first, 0)

    def other(i):
        blk_r, cr, blk_l, cl = came(i)
        return blk_r + 1 - 2 * core, cr, blk_l + 1 - 2 * core, cl

    def sib_wait(i):
        blk_r, cr, blk_l, cl = other(i)
        to_sib(blk_r, cr, sib_send.at[0, i], sib_recv.at[0, i]).wait_recv()
        to_sib(blk_l, cl, sib_send.at[1, i], sib_recv.at[1, i]).wait_recv()

    def pair(blk_a, ca, blk_b, cb):
        return (blk_a, ca), (blk_b, cb)

    def body(i, carry):
        comm(i)
        sib_wait(i - 1)
        attend(*pair(*other(i - 1)), *pair(*came(i)))
        return carry

    attend(*pair(*came(0)))
    lax.fori_loop(1, SENDS, body, 0)
    sib_wait(SENDS - 1)
    attend(*pair(*other(SENDS - 1)))

    total = jnp.zeros((8, C), F32)
    square = jnp.zeros((8, C), F32)
    for t in range(2):
        rows = pl.ds(256 * t, 256)
        inv = 1.0 / jnp.sum(l_s[rows, :], axis=1, keepdims=True)
        att = ((acc[rows, :] * inv - mean) * scale + shift).astype(BF16)
        x = jnp.concatenate([kv[me, 2 * t], kv[me, 2 * t + 1]], axis=0).astype(F32)
        h = (x + dot(att, wv[...])).astype(BF16)
        hid[2 * t] = h[:CH]
        hid[2 * t + 1] = h[CH:]
        h = h.astype(F32)
        if t == 0:
            base = h[0:1, :]
        a, b = sums_about(base, h)
        total = total + a
        square = square + b

    def halo_copy(k, row, peer):
        return pltpu.make_async_remote_copy(
            src_ref=hid.at[row],
            dst_ref=halo.at[k],
            send_sem=h_send.at[k],
            recv_sem=h_recv.at[k],
            device_id={"row": peer},
        )

    down = halo_copy(0, ROWS - 1, (me + 1) % DEV)
    up = halo_copy(1, 0, (me + DEV - 1) % DEV)
    put_moments(base, total, square, mine)
    for d in range(1, DEV):
        stat_copy(d, stat_b, sb_send, sb_recv).start()
    down.start()
    up.start()
    for c in taps:
        c.wait()
    down.wait()
    up.wait()
    for d in range(1, DEV):
        stat_copy(d, stat_b, sb_send, sb_recv).wait()
    mean2, rs2 = combined(stat_b, mine)
    coef[0] = mean2
    coef[1] = rs2 * vecs[2] * 0.5
    coef[2] = vecs[3] * 0.5
    edges[...] = halo[...]

    def drain(i, carry):
        blk_r, cr, blk_l, cl = came(i)
        ring(0, blk_r, cr, i).wait_send()
        ring(1, blk_l, cl, i).wait_send()
        to_sib(blk_r, cr, sib_send.at[0, i], sib_recv.at[0, i]).wait_send()
        to_sib(blk_l, cl, sib_send.at[1, i], sib_recv.at[1, i]).wait_send()
        return carry

    lax.fori_loop(0, SENDS, drain, 0)
    for i in range(4):
        to_sib(me, i, own_send.at[i], own_recv.at[i]).wait_send()


def conv_kernel(hid, edges, coef, wc, bias, out_ref, lhs):
    me = lax.axis_index("row")
    mean, scale, shift = coef[0], coef[1], coef[2]
    for j in range(ROWS + 2):
        src = edges[0] if j == 0 else edges[1] if j == ROWS + 1 else hid[j - 1]
        half = (src.astype(F32) - mean) * scale + shift
        act = half + half * jnp.tanh(half)
        if j == 0:
            act = jnp.where(me == 0, 0.0, act)
        if j == ROWS + 1:
            act = jnp.where(me == DEV - 1, 0.0, act)
        act = act.astype(BF16)
        for dy in range(3):
            i = j - dy
            if 0 <= i < ROWS:
                lhs[CH * i : CH * i + CH, C * dy : C * dy + C] = act

    col = lax.broadcasted_iota(jnp.int32, (N, 256), 0) % W
    for n in range(2):
        cols = slice(256 * n, 256 * n + 256)
        t0 = dot(lhs[...], wc[0, :, cols])
        t1 = dot(lhs[...], wc[1, :, cols])
        t2 = dot(lhs[...], wc[2, :, cols])
        total = t1 + jnp.where(col == 0, 0.0, pltpu.roll(t0, 1, 0))
        total = total + jnp.where(col == W - 1, 0.0, pltpu.roll(t2, N - 1, 0))
        base = jnp.concatenate([hid[i, :, cols] for i in range(4)], axis=0).astype(F32)
        out_ref[:, cols] = (base + (total + bias[:, cols])).astype(BF16)


def local(
    latent, attn_gain, attn_shift, w_query, w_key, w_value, w_out,
    conv_gain, conv_shift, w_conv, conv_bias,
):
    line = lambda v: v.reshape(1, C)
    dma = pltpu.SemaphoreType.DMA
    vmem = pl.BlockSpec(memory_space=pltpu.VMEM)
    hid, edges, coef, taps = pl.pallas_call(
        kernel,
        out_shape=(
            pltpu.VMEM((ROWS, W, C), BF16),
            pltpu.VMEM((2, W, C), BF16),
            pltpu.VMEM((3, 1, C), F32),
            pltpu.VMEM((3, 3 * C, C), BF16),
        ),
        in_specs=[pl.BlockSpec(memory_space=pltpu.HBM)] * 10,
        out_specs=(vmem,) * 4,
        scratch_shapes=[
            pltpu.VMEM((DEV, 4, CH, C), BF16),
            pltpu.VMEM((C, C), BF16),
            pltpu.VMEM((C, C), BF16),
            pltpu.VMEM((C, C), BF16),
            pltpu.VMEM((C, C), BF16),
            pltpu.VMEM((4, 1, C), F32),
            pltpu.VMEM((N, C), BF16),
            pltpu.VMEM((N, C), F32),
            pltpu.VMEM((N, 128), F32),
            pltpu.VMEM((N, 128), F32),
            pltpu.VMEM((2, W, C), BF16),
            pltpu.VMEM((8, 128), F32),
            pltpu.VMEM((DEV - 1, 8, 128), F32),
            pltpu.VMEM((DEV - 1, 8, 128), F32),
            dma((4,)),
            dma((4,)),
            dma((9,)),
            dma((4,)),
            dma((2, SENDS)),
            dma((2, SENDS)),
            dma((2, SENDS)),
            dma((2, SENDS)),
            dma((4,)),
            dma((4,)),
            dma((DEV - 1,)),
            dma((DEV - 1,)),
            dma((DEV - 1,)),
            dma((DEV - 1,)),
            dma((2,)),
            dma((2,)),
            pltpu.SemaphoreType.REGULAR((3,)),
        ],
        compiler_params=pltpu.CompilerParams(
            collective_id=0, has_side_effects=True, vmem_limit_bytes=28 * 1024 * 1024
        ),
    )(
        *(
            pltpu.with_memory_space_constraint(v, pltpu.HBM)
            for v in (
                latent.reshape(N, C), line(attn_gain), line(attn_shift), w_query, w_key,
                w_value, w_out, line(conv_gain), line(conv_shift), w_conv,
            )
        )
    )
    out = pl.pallas_call(
        conv_kernel,
        out_shape=jax.ShapeDtypeStruct((N, C), BF16),
        in_specs=[vmem] * 5,
        out_specs=vmem,
        scratch_shapes=[pltpu.VMEM((N, 3 * C), BF16)],
        compiler_params=pltpu.CompilerParams(vmem_limit_bytes=28 * 1024 * 1024),
    )(hid, edges, coef, taps, line(conv_bias))
    return out.reshape(ROWS, W, C)


def solution(mesh):
    part = P(("img", "row"), None, None)
    return jax.shard_map(
        local, mesh=mesh, in_specs=(part,) + (P(),) * 10, out_specs=part, check_vma=False
    )
```

```python
import jax
import jax.numpy as jnp
from jax import lax
from jax.experimental import pallas as pl
from jax.experimental.pallas import tpu as pltpu
from jax.sharding import PartitionSpec as P

C = 512
W = 128
ROWS = 4
N = ROWS * W
CH = 128
GROUP = 16
DEV = 16
ZN = 8
SENDS = 14
TILE = 256
SPLIT = 2
EPS = 1e-06
F32 = jnp.float32
BF16 = jnp.bfloat16
LOG2E = 1.4426950408889634

NT = (((1,), (1,)), ((), ()))


def dot(a, b, dims=(((1,), (0,)), ((), ()))):
    return lax.dot_general(a, b, dims, preferred_element_type=F32)


def as_rows(v):
    return jnp.concatenate([v[:, 128 * i : 128 * i + 128] for i in range(4)], axis=0)


def as_line(v):
    return jnp.concatenate([v[i : i + 1, :] for i in range(4)], axis=1)


def partner(v, step):
    lane = lax.broadcasted_iota(jnp.int32, v.shape, 1)
    return jnp.where(
        (lane // step) % 2 == 0, pltpu.roll(v, 128 - step, 1), pltpu.roll(v, step, 1)
    )


def slot(shape, first=0):
    lane = lax.broadcasted_iota(jnp.int32, shape, 1)
    return lane % GROUP == lax.broadcasted_iota(jnp.int32, shape, 0) + first


def put_moments(first, total, square, buf):
    total = jnp.sum(total, axis=0, keepdims=True)
    square = jnp.sum(square, axis=0, keepdims=True)
    off = total * (1.0 / N)
    dev = as_rows(jnp.maximum(square - total * off, 0.0))
    mean = as_rows(first + off)
    step, count = 1, float(N)
    while step < GROUP:
        other = partner(mean, step)
        gap = other - mean
        dev = dev + partner(dev, step) + (0.5 * count) * (gap * gap)
        mean = 0.5 * (mean + other)
        step, count = 2 * step, 2.0 * count
    line = jnp.where(slot(mean.shape), mean, 0.0) + jnp.where(slot(dev.shape, 4), dev, 0.0)
    buf[...] = jnp.sum(line, axis=0, keepdims=True)


def sums_about(first, block):
    off = (block - first).reshape(block.shape[0] // 8, 8, C)
    return jnp.sum(off, axis=0), jnp.sum(off * off, axis=0)


def combined(stats, own):
    lines = [own[...]] + [stats[i] for i in range(DEV - 1)]
    total = sum(lines[1:], lines[0])
    centre = total * (1.0 / DEV)
    spread = jnp.zeros((1, 128), F32)
    for v in lines:
        off = v - centre
        spread = spread + off * off
    spread = pltpu.roll(total, 128 - 4, 1) + float(N * GROUP) * spread
    rs = lax.rsqrt(spread * (1.0 / (DEV * GROUP * N)) + EPS)
    rows = [
        jnp.where(slot((4, 128)), jnp.broadcast_to(v, (4, 128)), 0.0) for v in (centre, rs)
    ]
    step = 1
    while step < GROUP:
        rows = [v + partner(v, step) for v in rows]
        step *= 2
    return tuple(as_line(v) for v in rows)


def kernel(
    x_hbm, ag_h, as_h, wq_h, wk_h, wv_h, wo_h, cg_h, cs_h, wc_h,
    hid, edges, coef, wc,
    kv, wq, wk, wv, wo, vecs, q_s, acc, m_s, l_s, halo, mine, stat_a, stat_b,
    load_sem, w_sem, wc_sem, v_sem,
    ring_send, ring_recv, sib_send, sib_recv, own_send, own_recv,
    sa_send, sa_recv, sb_send, sb_recv, h_send, h_recv, known,
):
    me = lax.axis_index("row")
    z = me // 2
    core = me % 2
    right = ((z + 1) % ZN) * 2 + core
    left = ((z + ZN - 1) % ZN) * 2 + core
    sib = z * 2 + (1 - core)

    loads = [
        pltpu.make_async_copy(x_hbm.at[pl.ds(CH * i, CH)], kv.at[me, i], load_sem.at[i])
        for i in range(4)
    ]
    for c in loads:
        c.start()

    barrier = pltpu.get_barrier_semaphore()
    for peer in (left, right, sib):
        pl.semaphore_signal(barrier, inc=1, device_id={"row": peer})

    small = [
        pltpu.make_async_copy(src, vecs.at[i], v_sem.at[i])
        for i, src in enumerate((ag_h, as_h, cg_h, cs_h))
    ]
    for c in small:
        c.start()
    weights = [
        pltpu.make_async_copy(src, dst, w_sem.at[i])
        for i, (src, dst) in enumerate(((wq_h, wq), (wk_h, wk), (wv_h, wv), (wo_h, wo)))
    ]
    for c in weights:
        c.start()
    taps = [
        pltpu.make_async_copy(
            wc_h.at[dy, dx], wc.at[dx, pl.ds(C * dy, C)], wc_sem.at[3 * dy + dx]
        )
        for dy in range(3)
        for dx in range(3)
    ]
    for c in taps:
        c.start()

    def ring(way, blk, chunk, j):
        return pltpu.make_async_remote_copy(
            src_ref=kv.at[blk, chunk],
            dst_ref=kv.at[blk, chunk],
            send_sem=ring_send.at[way, j],
            recv_sem=ring_recv.at[way, j],
            device_id={"row": right if way == 0 else left},
        )

    def to_sib(blk, chunk, sends, recvs):
        return pltpu.make_async_remote_copy(
            src_ref=kv.at[blk, chunk],
            dst_ref=kv.at[blk, chunk],
            send_sem=sends,
            recv_sem=recvs,
            device_id={"row": sib},
        )

    def stat_copy(d, dst, sends, recvs):
        return pltpu.make_async_remote_copy(
            src_ref=mine,
            dst_ref=dst.at[d - 1],
            send_sem=sends.at[d - 1],
            recv_sem=recvs.at[d - 1],
            device_id={"row": (me + d) % DEV},
        )

    pl.semaphore_wait(barrier, 3)

    order = ((0, 2), (1, 3), (2, 0), (3, 1))
    loads[0].wait()
    ring(0, me, 0, 0).start()
    loads[2].wait()
    ring(1, me, 2, 0).start()
    loads[1].wait()
    loads[3].wait()
    for j in range(1, 3):
        ring(0, me, order[j][0], j).start()
        ring(1, me, order[j][1], j).start()

    far_right = ((z + 2) % ZN) * 2 + core
    far_left = ((z + ZN - 2) % ZN) * 2 + core
    for k, peers in enumerate(((left, right, sib), (far_left, far_right), (sib,))):
        for peer in peers:
            pl.semaphore_signal(known.at[k], inc=1, device_id={"row": peer})
        if k == 0:
            base = kv[me, 0, 0:1, :].astype(F32)
            sums = [sums_about(base, kv[me, i].astype(F32)) for i in range(4)]
            put_moments(base, sum(a for a, _ in sums), sum(b for _, b in sums), mine)
        pl.semaphore_wait(known.at[k], len(peers))

    for d in range(1, DEV):
        stat_copy(d, stat_a, sa_send, sa_recv).start()
    for j in range(3, 4):
        ring(0, me, order[j][0], j).start()
        ring(1, me, order[j][1], j).start()
    for i in range(4):
        to_sib(me, i, own_send.at[i], own_recv.at[i]).start()

    m_s[...] = jnp.full_like(m_s, -1e30)
    l_s[...] = jnp.zeros_like(l_s)
    acc[...] = jnp.zeros_like(acc)

    for c in weights:
        c.wait()
    wv[...] = dot(wv[...], wo[...]).astype(BF16)

    def came(i):
        chunk = i % 4
        far = i // 4 + 1
        blk_r = ((z + ZN - far) % ZN) * 2 + core
        blk_l = ((z + far) % ZN) * 2 + core
        return blk_r, chunk, blk_l, (chunk + 2) % 4

    def comm(i):
        blk_r, cr, blk_l, cl = came(i)
        ring(0, blk_r, cr, i).wait_recv()
        ring(1, blk_l, cl, i).wait_recv()

        @pl.when(i < SENDS - 4)
        def _():
            ring(0, blk_r, cr, i + 4).start()
            ring(1, blk_l, cl, i + 4).start()

        to_sib(blk_r, cr, sib_send.at[0, i], sib_recv.at[0, i]).start()
        to_sib(blk_l, cl, sib_send.at[1, i], sib_recv.at[1, i]).start()

    def attend(*chunks):
        keys = jnp.concatenate([kv[blk, chunk] for blk, chunk in chunks], axis=0)
        spans = range(0, CH * len(chunks), 128)

        def weigh(rows, s):
            m_old = m_s[rows, :]
            m_new = jnp.maximum(m_old, jnp.max(s, axis=1, keepdims=True))
            alpha = jnp.exp2(m_old - m_new)
            p = [jnp.exp2(s[:, k : k + 128] - m_new).astype(BF16) for k in spans]
            l_s[rows, :] = l_s[rows, :] * alpha + sum(v.astype(F32) for v in p)
            m_s[rows, :] = m_new
            return jnp.concatenate([alpha] * 4, axis=1), jnp.concatenate(p, axis=1)

        tiles = [pl.ds(TILE * t, TILE) for t in range(N // TILE)]
        s = dot(q_s[tiles[0], :], keys, NT)
        for t, rows in enumerate(tiles):
            ahead = dot(q_s[tiles[t + 1], :], keys, NT) if t + 1 < len(tiles) else None
            alpha, p = weigh(rows, s)
            acc[rows, :] = acc[rows, :] * alpha + dot(p, keys)
            s = ahead

    comm(0)

    for c in small:
        c.wait()
    for d in range(1, DEV):
        stat_copy(d, stat_a, sa_send, sa_recv).wait()
    comm(1)
    mean, rs = combined(stat_a, mine)
    scale = rs * vecs[0]
    shift = vecs[1]
    for i in range(4):
        normed = ((kv[me, i].astype(F32) - mean) * scale + shift).astype(BF16)
        query = dot(normed, wq[...]).astype(BF16)
        folded = dot(query, wk[...], NT) * (scale * (LOG2E / C**0.5))
        q_s[CH * i : CH * i + CH, :] = folded.astype(BF16)

    for i in range(4):
        to_sib(me, i, own_send.at[i], own_recv.at[i]).wait_recv()

    def first(k, carry):
        blk = jnp.where(k < 1, me, sib)
        attend((blk, 0), (blk, 1), (blk, 2), (blk, 3))
        return carry

    lax.fori_loop(0, 2, first, 0)

    def other(i):
        blk_r, cr, blk_l, cl = came(i)
        return blk_r + 1 - 2 * core, cr, blk_l + 1 - 2 * core, cl

    def sib_wait(i):
        blk_r, cr, blk_l, cl = other(i)
        to_sib(blk_r, cr, sib_send.at[0, i], sib_recv.at[0, i]).wait_recv()
        to_sib(blk_l, cl, sib_send.at[1, i], sib_recv.at[1, i]).wait_recv()

    def pair(blk_a, ca, blk_b, cb):
        return (blk_a, ca), (blk_b, cb)

    def body(i, carry):
        pl.when(i > 2)(lambda: comm(i))
        sib_wait(i - 1)
        attend(*pair(*other(i - 1)), *pair(*came(i)))
        return carry

    comm(2)
    attend(*pair(*came(0)))
    lax.fori_loop(1, SENDS, body, 0)
    sib_wait(SENDS - 1)
    attend(*pair(*other(SENDS - 1)))

    def halo_copy(k, part):
        row, peer = ((ROWS - 1, (me + 1) % DEV), (0, (me + DEV - 1) % DEV))[k]
        piece = pl.ds(part * (W // 2), W // 2)
        return pltpu.make_async_remote_copy(
            src_ref=hid.at[row, piece],
            dst_ref=halo.at[k, piece],
            send_sem=h_send.at[k, part],
            recv_sem=h_recv.at[k, part],
            device_id={"row": peer},
        )

    total = jnp.zeros((8, C), F32)
    square = jnp.zeros((8, C), F32)
    for pair_rows in ((0, 3), (1, 2)):
        spans = [pl.ds(W * r, W) for r in pair_rows]
        den = jnp.concatenate([l_s[rows, :] for rows in spans], axis=0)
        inv = 1.0 / jnp.sum(den, axis=1, keepdims=True)
        got = jnp.concatenate([acc[rows, :] for rows in spans], axis=0)
        att = ((got * inv - mean) * scale + shift).astype(BF16)
        x = jnp.concatenate([kv[me, r] for r in pair_rows], axis=0).astype(F32)
        h = (x + dot(att, wv[...])).astype(BF16)
        hid[pair_rows[0]] = h[:W]
        hid[pair_rows[1]] = h[W:]
        h = h.astype(F32)
        if pair_rows[0] == 0:
            base = h[0:1, :]
            for k in range(2):
                halo_copy(k, 0).start()
        a, b = sums_about(base, h)
        total = total + a
        square = square + b

    put_moments(base, total, square, mine)
    for d in range(1, DEV):
        stat_copy(d, stat_b, sb_send, sb_recv).start()
    for k in range(2):
        halo_copy(k, 1).start()
    for c in taps:
        c.wait()
    for k in range(2):
        for part in range(2):
            halo_copy(k, part).wait()
    for d in range(1, DEV):
        stat_copy(d, stat_b, sb_send, sb_recv).wait()
    mean2, rs2 = combined(stat_b, mine)
    coef[0] = mean2
    coef[1] = rs2 * vecs[2] * 0.5
    coef[2] = vecs[3] * 0.5
    edges[...] = halo[...]

    def drain(i, carry):
        blk_r, cr, blk_l, cl = came(i)
        ring(0, blk_r, cr, i).wait_send()
        ring(1, blk_l, cl, i).wait_send()
        to_sib(blk_r, cr, sib_send.at[0, i], sib_recv.at[0, i]).wait_send()
        to_sib(blk_l, cl, sib_send.at[1, i], sib_recv.at[1, i]).wait_send()
        return carry

    lax.fori_loop(0, SENDS, drain, 0)
    for i in range(4):
        to_sib(me, i, own_send.at[i], own_recv.at[i]).wait_send()


def conv_kernel(hid, edges, coef, wc, bias, out_hbm, act_s, out_s, out_sem):
    me = lax.axis_index("row")
    mean, scale, shift = coef[0], coef[1], coef[2]

    def activate(j):
        src = edges[0] if j == 0 else edges[1] if j == ROWS + 1 else hid[j - 1]
        half = (src.astype(F32) - mean) * scale + shift
        act = half + half * jnp.tanh(half)
        if j == 0:
            act = jnp.where(me == 0, 0.0, act)
        if j == ROWS + 1:
            act = jnp.where(me == DEV - 1, 0.0, act)
        act_s[W * j : W * j + W, :] = act.astype(BF16)

    part = N // SPLIT
    col = lax.broadcasted_iota(jnp.int32, (part, C), 0) % W
    ready = 0
    copies = []
    for m in range(SPLIT):
        rows = slice(part * m, part * m + part)
        while ready * W < part * m + part + 2 * W:
            activate(ready)
            ready += 1
        t = [
            sum(
                dot(act_s[part * m + W * dy : part * m + W * dy + part, :], wc[dx, C * dy : C * dy + C])
                for dy in range(3)
            )
            for dx in range(3)
        ]
        total = t[1] + jnp.where(col == 0, 0.0, pltpu.roll(t[0], 1, 0))
        total = total + jnp.where(col == W - 1, 0.0, pltpu.roll(t[2], part - 1, 0))
        first = part // W * m
        base = jnp.concatenate([hid[first + i] for i in range(part // W)], axis=0).astype(F32)
        out_s[rows, :] = (base + (total + bias[...])).astype(BF16)
        copies.append(pltpu.make_async_copy(out_s.at[rows], out_hbm.at[rows], out_sem.at[m]))
        copies[-1].start()
    for c in copies:
        c.wait()


def local(
    latent, attn_gain, attn_shift, w_query, w_key, w_value, w_out,
    conv_gain, conv_shift, w_conv, conv_bias,
):
    line = lambda v: v.reshape(1, C)
    dma = pltpu.SemaphoreType.DMA
    vmem = pl.BlockSpec(memory_space=pltpu.VMEM)
    hid, edges, coef, taps = pl.pallas_call(
        kernel,
        out_shape=(
            pltpu.VMEM((ROWS, W, C), BF16),
            pltpu.VMEM((2, W, C), BF16),
            pltpu.VMEM((3, 1, C), F32),
            pltpu.VMEM((3, 3 * C, C), BF16),
        ),
        in_specs=[pl.BlockSpec(memory_space=pltpu.HBM)] * 10,
        out_specs=(vmem,) * 4,
        scratch_shapes=[
            pltpu.VMEM((DEV, 4, CH, C), BF16),
            pltpu.VMEM((C, C), BF16),
            pltpu.VMEM((C, C), BF16),
            pltpu.VMEM((C, C), BF16),
            pltpu.VMEM((C, C), BF16),
            pltpu.VMEM((4, 1, C), F32),
            pltpu.VMEM((N, C), BF16),
            pltpu.VMEM((N, C), F32),
            pltpu.VMEM((N, 128), F32),
            pltpu.VMEM((N, 128), F32),
            pltpu.VMEM((2, W, C), BF16),
            pltpu.VMEM((1, 128), F32),
            pltpu.VMEM((DEV - 1, 1, 128), F32),
            pltpu.VMEM((DEV - 1, 1, 128), F32),
            dma((4,)),
            dma((4,)),
            dma((9,)),
            dma((4,)),
            dma((2, SENDS)),
            dma((2, SENDS)),
            dma((2, SENDS)),
            dma((2, SENDS)),
            dma((4,)),
            dma((4,)),
            dma((DEV - 1,)),
            dma((DEV - 1,)),
            dma((DEV - 1,)),
            dma((DEV - 1,)),
            dma((2, 2)),
            dma((2, 2)),
            pltpu.SemaphoreType.REGULAR((3,)),
        ],
        compiler_params=pltpu.CompilerParams(
            collective_id=0, has_side_effects=True, vmem_limit_bytes=28 * 1024 * 1024
        ),
    )(
        *(
            pltpu.with_memory_space_constraint(v, pltpu.HBM)
            for v in (
                latent.reshape(N, C), line(attn_gain), line(attn_shift), w_query, w_key,
                w_value, w_out, line(conv_gain), line(conv_shift), w_conv,
            )
        )
    )
    out = pl.pallas_call(
        conv_kernel,
        out_shape=jax.ShapeDtypeStruct((N, C), BF16),
        in_specs=[vmem] * 5,
        out_specs=pl.BlockSpec(memory_space=pltpu.HBM),
        scratch_shapes=[
            pltpu.VMEM((N + 2 * W, C), BF16),
            pltpu.VMEM((N, C), BF16),
            dma((SPLIT,)),
        ],
        compiler_params=pltpu.CompilerParams(vmem_limit_bytes=28 * 1024 * 1024),
    )(hid, edges, coef, taps, line(conv_bias))
    return out.reshape(ROWS, W, C)


def solution(mesh):
    part = P(("img", "row"), None, None)
    return jax.shard_map(
        local, mesh=mesh, in_specs=(part,) + (P(),) * 10, out_specs=part, check_vma=False
    )
```

```python
import jax
import jax.numpy as jnp
from jax import lax
from jax.experimental import pallas as pl
from jax.experimental.pallas import tpu as pltpu
from jax.sharding import PartitionSpec as P

C = 512
W = 128
ROWS = 4
N = ROWS * W
CH = 128
GROUP = 16
DEV = 16
ZN = 8
SENDS = 14
TILE = 256
SPLIT = 2
FEW = 16
NEAREST = sorted(range(1, DEV), key=lambda d: min(d, DEV - d))
EPS = 1e-06
F32 = jnp.float32
BF16 = jnp.bfloat16
LOG2E = 1.4426950408889634

NT = (((1,), (1,)), ((), ()))


def dot(a, b, dims=(((1,), (0,)), ((), ()))):
    return lax.dot_general(a, b, dims, preferred_element_type=F32)


def as_rows(v):
    return jnp.concatenate([v[:, 128 * i : 128 * i + 128] for i in range(4)], axis=0)


def as_line(v):
    return jnp.concatenate([v[i : i + 1, :] for i in range(4)], axis=1)


def partner(v, step):
    lane = lax.broadcasted_iota(jnp.int32, v.shape, 1)
    return jnp.where(
        (lane // step) % 2 == 0, pltpu.roll(v, 128 - step, 1), pltpu.roll(v, step, 1)
    )


def slot(shape, first=0):
    lane = lax.broadcasted_iota(jnp.int32, shape, 1)
    return lane % GROUP == lax.broadcasted_iota(jnp.int32, shape, 0) + first


def put_moments(first, total, square, buf):
    total = jnp.sum(total, axis=0, keepdims=True)
    square = jnp.sum(square, axis=0, keepdims=True)
    off = total * (1.0 / N)
    dev = as_rows(jnp.maximum(square - total * off, 0.0))
    mean = as_rows(first + off)
    step, count = 1, float(N)
    while step < GROUP:
        other = partner(mean, step)
        gap = other - mean
        dev = dev + partner(dev, step) + (0.5 * count) * (gap * gap)
        mean = 0.5 * (mean + other)
        step, count = 2 * step, 2.0 * count
    line = jnp.where(slot(mean.shape), mean, 0.0) + jnp.where(slot(dev.shape, 4), dev, 0.0)
    buf[...] = jnp.sum(line, axis=0, keepdims=True)


def sums_about(first, block):
    off = (block - first).reshape(block.shape[0] // 8, 8, C)
    return jnp.sum(off, axis=0), jnp.sum(off * off, axis=0)


def combined(stats, own):
    lines = [own[...]] + [stats[i] for i in range(DEV - 1)]
    total = sum(lines[1:], lines[0])
    centre = total * (1.0 / DEV)
    spread = jnp.zeros((1, 128), F32)
    for v in lines:
        off = v - centre
        spread = spread + off * off
    spread = pltpu.roll(total, 128 - 4, 1) + float(N * GROUP) * spread
    rs = lax.rsqrt(spread * (1.0 / (DEV * GROUP * N)) + EPS)
    rows = [
        jnp.where(slot((4, 128)), jnp.broadcast_to(v, (4, 128)), 0.0) for v in (centre, rs)
    ]
    step = 1
    while step < GROUP:
        rows = [v + partner(v, step) for v in rows]
        step *= 2
    return tuple(as_line(v) for v in rows)


def kernel(
    x_hbm, ag_h, as_h, wq_h, wk_h, wv_h, wo_h, cg_h, cs_h, wc_h,
    hid, edges, coef, wc,
    kv, wq, wk, wv, wo, mid, vecs, q_s, acc, m_s, l_s, halo, mine, stat_a, stat_b,
    load_sem, w_sem, wc_sem, v_sem,
    ring_send, ring_recv, sib_send, sib_recv, own_send, own_recv,
    sa_send, sa_recv, sb_send, sb_recv, h_send, h_recv, known,
):
    me = lax.axis_index("row")
    z = me // 2
    core = me % 2
    right = ((z + 1) % ZN) * 2 + core
    left = ((z + ZN - 1) % ZN) * 2 + core
    sib = z * 2 + (1 - core)

    loads = [
        pltpu.make_async_copy(x_hbm.at[pl.ds(CH * i, CH)], kv.at[me, i], load_sem.at[i])
        for i in range(4)
    ]
    barrier = pltpu.get_barrier_semaphore()
    for peer in (left, right, sib):
        pl.semaphore_signal(barrier, inc=1, device_id={"row": peer})
    for c in loads:
        c.start()

    small = [
        pltpu.make_async_copy(src, vecs.at[i], v_sem.at[i])
        for i, src in enumerate((ag_h, as_h, cg_h, cs_h))
    ]
    weights = [
        pltpu.make_async_copy(src, dst, w_sem.at[i])
        for i, (src, dst) in enumerate(((wq_h, wq), (wk_h, wk), (wv_h, wv), (wo_h, wo)))
    ]
    taps = [
        pltpu.make_async_copy(
            wc_h.at[dy, dx], (wc.at[dx, 0], mid.at[dx], wc.at[dx, 3])[dy], wc_sem.at[3 * dy + dx]
        )
        for dy in range(3)
        for dx in range(3)
    ]

    def ring(way, blk, chunk, j):
        return pltpu.make_async_remote_copy(
            src_ref=kv.at[blk, chunk],
            dst_ref=kv.at[blk, chunk],
            send_sem=ring_send.at[way, j],
            recv_sem=ring_recv.at[way, j],
            device_id={"row": right if way == 0 else left},
        )

    def to_sib(blk, chunk, sends, recvs):
        return pltpu.make_async_remote_copy(
            src_ref=kv.at[blk, chunk],
            dst_ref=kv.at[blk, chunk],
            send_sem=sends,
            recv_sem=recvs,
            device_id={"row": sib},
        )

    def stat_copy(d, dst, sends, recvs):
        return pltpu.make_async_remote_copy(
            src_ref=mine,
            dst_ref=dst.at[d - 1],
            send_sem=sends.at[d - 1],
            recv_sem=recvs.at[d - 1],
            device_id={"row": (me + d) % DEV},
        )

    pl.semaphore_wait(barrier, 3)

    order = ((0, 2), (1, 3), (2, 0), (3, 1))
    loads[0].wait()
    ring(0, me, 0, 0).start()
    loads[2].wait()
    ring(1, me, 2, 0).start()
    loads[1].wait()
    loads[3].wait()
    for j in range(1, 3):
        ring(0, me, order[j][0], j).start()
        ring(1, me, order[j][1], j).start()

    for c in (*small, *weights):
        c.start()

    far_right = ((z + 2) % ZN) * 2 + core
    far_left = ((z + ZN - 2) % ZN) * 2 + core
    for k, peers in enumerate(((left, right, sib), (far_left, far_right), (sib,))):
        for peer in peers:
            pl.semaphore_signal(known.at[k], inc=1, device_id={"row": peer})
        if k == 0:
            base = kv[me, 0, 0:1, :].astype(F32)
            sums = [sums_about(base, kv[me, i].astype(F32)) for i in range(4)]
            put_moments(base, sum(a for a, _ in sums), sum(b for _, b in sums), mine)
        pl.semaphore_wait(known.at[k], len(peers))

    for d in range(1, DEV):
        stat_copy(d, stat_a, sa_send, sa_recv).start()
    for j in range(3, 4):
        ring(0, me, order[j][0], j).start()
        ring(1, me, order[j][1], j).start()
    for i in range(4):
        to_sib(me, i, own_send.at[i], own_recv.at[i]).start()

    m_s[...] = jnp.full_like(m_s, -1e30)
    l_s[...] = jnp.zeros_like(l_s)
    acc[...] = jnp.zeros_like(acc)

    for c in weights:
        c.wait()
    wv[...] = dot(wv[...], wo[...]).astype(BF16)

    def came(i):
        chunk = i % 4
        far = i // 4 + 1
        blk_r = ((z + ZN - far) % ZN) * 2 + core
        blk_l = ((z + far) % ZN) * 2 + core
        return blk_r, chunk, blk_l, (chunk + 2) % 4

    def comm(i):
        blk_r, cr, blk_l, cl = came(i)
        for way, blk, chunk in ((0, blk_r, cr), (1, blk_l, cl)):
            ring(way, blk, chunk, i).wait_recv()

            @pl.when(i < SENDS - 4)
            def _():
                ring(way, blk, chunk, i + 4).start()

            to_sib(blk, chunk, sib_send.at[way, i], sib_recv.at[way, i]).start()

    def attend(*chunks):
        keys = jnp.concatenate([kv[blk, chunk] for blk, chunk in chunks], axis=0)
        spans = range(0, CH * len(chunks), 128)

        def weigh(rows, s):
            m_old = m_s[rows, :]
            m_new = jnp.maximum(m_old, jnp.max(s, axis=1, keepdims=True))
            alpha = jnp.exp2(m_old - m_new)
            p = [jnp.exp2(s[:, k : k + 128] - m_new).astype(BF16) for k in spans]
            l_s[rows, :] = l_s[rows, :] * alpha + sum(v.astype(F32) for v in p)
            m_s[rows, :] = m_new
            return jnp.concatenate([alpha] * 4, axis=1), jnp.concatenate(p, axis=1)

        tiles = [pl.ds(TILE * t, TILE) for t in range(N // TILE)]
        s = dot(q_s[tiles[0], :], keys, NT)
        for t, rows in enumerate(tiles):
            ahead = dot(q_s[tiles[t + 1], :], keys, NT) if t + 1 < len(tiles) else None
            alpha, p = weigh(rows, s)
            acc[rows, :] = acc[rows, :] * alpha + dot(p, keys)
            s = ahead

    comm(0)

    for c in small:
        c.wait()
    for d in range(1, DEV):
        stat_copy(d, stat_a, sa_send, sa_recv).wait()
    comm(1)
    mean, rs = combined(stat_a, mine)
    scale = rs * vecs[0]
    shift = vecs[1]
    for i in range(4):
        normed = ((kv[me, i].astype(F32) - mean) * scale + shift).astype(BF16)
        query = dot(normed, wq[...]).astype(BF16)
        folded = dot(query, wk[...], NT) * (scale * (LOG2E / C**0.5))
        q_s[CH * i : CH * i + CH, :] = folded.astype(BF16)

    for i in range(4):
        to_sib(me, i, own_send.at[i], own_recv.at[i]).wait_recv()

    def first(k, carry):
        blk = jnp.where(k < 1, me, sib)
        attend((blk, 0), (blk, 1), (blk, 2), (blk, 3))
        return carry

    for c in taps:
        c.start()
    lax.fori_loop(0, 2, first, 0)

    def other(i):
        blk_r, cr, blk_l, cl = came(i)
        return blk_r + 1 - 2 * core, cr, blk_l + 1 - 2 * core, cl

    def sib_wait(i):
        blk_r, cr, blk_l, cl = other(i)
        to_sib(blk_r, cr, sib_send.at[0, i], sib_recv.at[0, i]).wait_recv()
        to_sib(blk_l, cl, sib_send.at[1, i], sib_recv.at[1, i]).wait_recv()

    def pair(blk_a, ca, blk_b, cb):
        return (blk_a, ca), (blk_b, cb)

    def spread_taps(k):
        dx, rows = k // 8, pl.ds(pl.multiple_of(k % 8 * 64, 64), 64)
        ends = (wc[dx, 0, rows, :].astype(F32) + wc[dx, 3, rows, :].astype(F32)) * -0.5
        half = mid[dx, rows, :].astype(F32) * -0.5
        wc[dx, 1, rows, :] = (ends + half).astype(BF16)
        wc[dx, 2, rows, :] = (ends - half).astype(BF16)

    for c in taps:
        c.wait()

    def body(i, carry):
        @pl.when(i < 13)
        def _():
            spread_taps(2 * i - 2)
            spread_taps(2 * i - 1)

        pl.when(i > 2)(lambda: comm(i))
        sib_wait(i - 1)
        attend(*pair(*other(i - 1)), *pair(*came(i)))
        return carry

    comm(2)
    attend(*pair(*came(0)))
    lax.fori_loop(1, SENDS, body, 0)
    sib_wait(SENDS - 1)
    attend(*pair(*other(SENDS - 1)))

    def halo_copy(k, part):
        row, peer = ((ROWS - 1, (me + 1) % DEV), (0, (me + DEV - 1) % DEV))[k]
        piece = pl.ds(part * (W // 2), W // 2)
        return pltpu.make_async_remote_copy(
            src_ref=hid.at[row, piece],
            dst_ref=halo.at[k, piece],
            send_sem=h_send.at[k, part],
            recv_sem=h_recv.at[k, part],
            device_id={"row": peer},
        )

    total = jnp.zeros((8, C), F32)
    square = jnp.zeros((8, C), F32)
    for pair_rows in ((0, 3), (1, 2)):
        spans = [pl.ds(W * r, W) for r in pair_rows]
        den = jnp.concatenate([l_s[rows, :] for rows in spans], axis=0)
        inv = 1.0 / jnp.sum(den, axis=1, keepdims=True)
        got = jnp.concatenate([acc[rows, :] for rows in spans], axis=0)
        att = ((got * inv - mean) * scale + shift).astype(BF16)
        x = jnp.concatenate([kv[me, r] for r in pair_rows], axis=0).astype(F32)
        h = (x + dot(att, wv[...])).astype(BF16)
        hid[pair_rows[0]] = h[:W]
        hid[pair_rows[1]] = h[W:]
        h = h.astype(F32)
        if pair_rows[0] == 0:
            base = h[0:1, :]
            for k in range(2):
                halo_copy(k, 0).start()
        a, b = sums_about(base, h)
        total = total + a
        square = square + b

    put_moments(base, total, square, mine)
    for d in range(1, DEV):
        stat_copy(d, stat_b, sb_send, sb_recv).start()
    for k in range(2):
        halo_copy(k, 1).start()
    def drain(i, carry):
        blk_r, cr, blk_l, cl = came(i)
        ring(0, blk_r, cr, i).wait_send()
        ring(1, blk_l, cl, i).wait_send()
        to_sib(blk_r, cr, sib_send.at[0, i], sib_recv.at[0, i]).wait_send()
        to_sib(blk_l, cl, sib_send.at[1, i], sib_recv.at[1, i]).wait_send()
        return carry

    lax.fori_loop(0, SENDS, drain, 0)
    for i in range(4):
        to_sib(me, i, own_send.at[i], own_recv.at[i]).wait_send()

    for k in range(2):
        for part in range(2):
            halo_copy(k, part).wait_send()
    for d in range(1, DEV):
        stat_copy(d, stat_b, sb_send, sb_recv).wait_send()
    for d in NEAREST:
        stat_copy(d, stat_b, sb_send, sb_recv).wait_recv()
    for k in range(2):
        for part in range(2):
            halo_copy(k, part).wait_recv()
    edges[...] = halo[...]
    mean2, rs2 = combined(stat_b, mine)
    coef[0] = mean2
    coef[1] = rs2 * vecs[2] * 0.5
    coef[2] = vecs[3] * 0.5


def conv_kernel(hid, edges, coef, wc, bias, out_hbm, mix_s, out_s, out_sem):
    me = lax.axis_index("row")
    mean, scale, shift = coef[0], coef[1], coef[2]

    for lo in range(0, W, FEW):
        d = []
        for j in range(ROWS + 2):
            src, r = (edges, 0) if j == 0 else (edges, 1) if j == ROWS + 1 else (hid, j - 1)
            half = (src[r, lo : lo + FEW, :].astype(F32) - mean) * scale + shift
            act = half + half * jnp.tanh(half)
            if j == 0:
                act = jnp.where(me == 0, 0.0, act)
            if j == ROWS + 1:
                act = jnp.where(me == DEV - 1, 0.0, act)
            d.append(act.astype(BF16))
        for a in range(2):
            e = d[2 * a : 2 * a + 4]
            for k, v in ((1, e[1] + e[2]), (2, e[2] - e[1]), (0, e[0] - e[2]), (3, e[1] - e[3])):
                mix_s[k, W * a + lo : W * a + lo + FEW, :] = v

    part = C // SPLIT
    col = lax.broadcasted_iota(jnp.int32, (2 * W, part), 0) % W
    copies = []
    for n in range(SPLIT):
        cols = slice(part * n, part * n + part)
        rows = [None, None]
        for dx in (1, 0, 2):
            m = [None] * 4
            for k in (1, 2, 0, 3):
                m[k] = dot(mix_s[k], wc[dx, k, :, cols])
            for i, v in enumerate((m[0] - m[1] - m[2], m[2] - m[1] - m[3])):
                if dx == 0:
                    v = jnp.where(col == 0, 0.0, pltpu.roll(v, 1, 0))
                if dx == 2:
                    v = jnp.where(col == W - 1, 0.0, pltpu.roll(v, 2 * W - 1, 0))
                rows[i] = v if rows[i] is None else rows[i] + v
        for r in range(ROWS):
            total = rows[r % 2][W * (r // 2) : W * (r // 2) + W]
            base = hid[r, :, cols].astype(F32)
            out_s[W * r : W * r + W, cols] = (base + (total + bias[:, cols])).astype(BF16)
        copies.append(
            pltpu.make_async_copy(out_s.at[:, cols], out_hbm.at[:, cols], out_sem.at[n])
        )
        copies[-1].start()
    for c in copies:
        c.wait()


def local(
    latent, attn_gain, attn_shift, w_query, w_key, w_value, w_out,
    conv_gain, conv_shift, w_conv, conv_bias,
):
    line = lambda v: v.reshape(1, C)
    dma = pltpu.SemaphoreType.DMA
    vmem = pl.BlockSpec(memory_space=pltpu.VMEM)
    hid, edges, coef, taps = pl.pallas_call(
        kernel,
        out_shape=(
            pltpu.VMEM((ROWS, W, C), BF16),
            pltpu.VMEM((2, W, C), BF16),
            pltpu.VMEM((3, 1, C), F32),
            pltpu.VMEM((3, 4, C, C), BF16),
        ),
        in_specs=[pl.BlockSpec(memory_space=pltpu.HBM)] * 10,
        out_specs=(vmem,) * 4,
        scratch_shapes=[
            pltpu.VMEM((DEV, 4, CH, C), BF16),
            pltpu.VMEM((C, C), BF16),
            pltpu.VMEM((C, C), BF16),
            pltpu.VMEM((C, C), BF16),
            pltpu.VMEM((C, C), BF16),
            pltpu.VMEM((3, C, C), BF16),
            pltpu.VMEM((4, 1, C), F32),
            pltpu.VMEM((N, C), BF16),
            pltpu.VMEM((N, C), F32),
            pltpu.VMEM((N, 128), F32),
            pltpu.VMEM((N, 128), F32),
            pltpu.VMEM((2, W, C), BF16),
            pltpu.VMEM((1, 128), F32),
            pltpu.VMEM((DEV - 1, 1, 128), F32),
            pltpu.VMEM((DEV - 1, 1, 128), F32),
            dma((4,)),
            dma((4,)),
            dma((9,)),
            dma((4,)),
            dma((2, SENDS)),
            dma((2, SENDS)),
            dma((2, SENDS)),
            dma((2, SENDS)),
            dma((4,)),
            dma((4,)),
            dma((DEV - 1,)),
            dma((DEV - 1,)),
            dma((DEV - 1,)),
            dma((DEV - 1,)),
            dma((2, 2)),
            dma((2, 2)),
            pltpu.SemaphoreType.REGULAR((3,)),
        ],
        compiler_params=pltpu.CompilerParams(
            collective_id=0, has_side_effects=True, vmem_limit_bytes=30 * 1024 * 1024
        ),
    )(
        *(
            pltpu.with_memory_space_constraint(v, pltpu.HBM)
            for v in (
                latent.reshape(N, C), line(attn_gain), line(attn_shift), w_query, w_key,
                w_value, w_out, line(conv_gain), line(conv_shift), w_conv,
            )
        )
    )
    out = pl.pallas_call(
        conv_kernel,
        out_shape=jax.ShapeDtypeStruct((N, C), BF16),
        in_specs=[vmem] * 5,
        out_specs=pl.BlockSpec(memory_space=pltpu.HBM),
        scratch_shapes=[
            pltpu.VMEM((4, 2 * W, C), BF16),
            pltpu.VMEM((N, C), BF16),
            dma((SPLIT,)),
        ],
        compiler_params=pltpu.CompilerParams(vmem_limit_bytes=28 * 1024 * 1024),
    )(hid, edges, coef, taps, line(conv_bias))
    return out.reshape(ROWS, W, C)


def solution(mesh):
    part = P(("img", "row"), None, None)
    return jax.shard_map(
        local, mesh=mesh, in_specs=(part,) + (P(),) * 10, out_specs=part, check_vma=False
    )
```

```python
import jax
import jax.numpy as jnp
from jax import lax
from jax.experimental import pallas as pl
from jax.experimental.pallas import tpu as pltpu
from jax.sharding import PartitionSpec as P

C = 512
W = 128
ROWS = 4
N = ROWS * W
CH = 128
GROUP = 16
DEV = 16
ZN = 8
SENDS = 14
TILE = 256
SPLIT = 2
FEW = 16
NEAREST = sorted(range(1, DEV), key=lambda d: min(d, DEV - d))
EPS = 1e-06
F32 = jnp.float32
BF16 = jnp.bfloat16
LOG2E = 1.4426950408889634

NT = (((1,), (1,)), ((), ()))


def dot(a, b, dims=(((1,), (0,)), ((), ()))):
    return lax.dot_general(a, b, dims, preferred_element_type=F32)


def as_rows(v):
    return jnp.concatenate([v[:, 128 * i : 128 * i + 128] for i in range(4)], axis=0)


def as_line(v):
    return jnp.concatenate([v[i : i + 1, :] for i in range(4)], axis=1)


def partner(v, step):
    lane = lax.broadcasted_iota(jnp.int32, v.shape, 1)
    return jnp.where(
        (lane // step) % 2 == 0, pltpu.roll(v, 128 - step, 1), pltpu.roll(v, step, 1)
    )


def slot(shape, first=0):
    lane = lax.broadcasted_iota(jnp.int32, shape, 1)
    return lane % GROUP == lax.broadcasted_iota(jnp.int32, shape, 0) + first


def put_moments(first, total, square, buf):
    total = jnp.sum(total, axis=0, keepdims=True)
    square = jnp.sum(square, axis=0, keepdims=True)
    off = total * (1.0 / N)
    dev = as_rows(jnp.maximum(square - total * off, 0.0))
    mean = as_rows(first + off)
    step, count = 1, float(N)
    while step < GROUP:
        other = partner(mean, step)
        gap = other - mean
        dev = dev + partner(dev, step) + (0.5 * count) * (gap * gap)
        mean = 0.5 * (mean + other)
        step, count = 2 * step, 2.0 * count
    line = jnp.where(slot(mean.shape), mean, 0.0) + jnp.where(slot(dev.shape, 4), dev, 0.0)
    buf[...] = jnp.sum(line, axis=0, keepdims=True)


def sums_about(first, block):
    off = (block - first).reshape(block.shape[0] // 8, 8, C)
    return jnp.sum(off, axis=0), jnp.sum(off * off, axis=0)


def combined(stats, own):
    lines = [own[...]] + [stats[i] for i in range(DEV - 1)]
    total = sum(lines[1:], lines[0])
    centre = total * (1.0 / DEV)
    spread = jnp.zeros((1, 128), F32)
    for v in lines:
        off = v - centre
        spread = spread + off * off
    spread = pltpu.roll(total, 128 - 4, 1) + float(N * GROUP) * spread
    rs = lax.rsqrt(spread * (1.0 / (DEV * GROUP * N)) + EPS)
    rows = [
        jnp.where(slot((4, 128)), jnp.broadcast_to(v, (4, 128)), 0.0) for v in (centre, rs)
    ]
    step = 1
    while step < GROUP:
        rows = [v + partner(v, step) for v in rows]
        step *= 2
    return tuple(as_line(v) for v in rows)


def kernel(
    x_hbm, ag_h, as_h, wq_h, wk_h, wv_h, wo_h, cg_h, cs_h, wc_h,
    hid, edges, coef, wc,
    kv, wq, wk, wv, wo, mid, vecs, q_s, acc, m_s, l_s, halo, mine, stat_a, stat_b,
    load_sem, w_sem, wc_sem, v_sem,
    ring_send, ring_recv, sib_send, sib_recv, own_send, own_recv,
    sa_send, sa_recv, sb_send, sb_recv, h_send, h_recv, known,
):
    me = lax.axis_index("row")
    z = me // 2
    core = me % 2
    right = ((z + 1) % ZN) * 2 + core
    left = ((z + ZN - 1) % ZN) * 2 + core
    sib = z * 2 + (1 - core)

    loads = [
        pltpu.make_async_copy(x_hbm.at[pl.ds(CH * i, CH)], kv.at[me, i], load_sem.at[i])
        for i in range(4)
    ]
    barrier = pltpu.get_barrier_semaphore()
    for peer in (left, right, sib):
        pl.semaphore_signal(barrier, inc=1, device_id={"row": peer})
    for c in loads:
        c.start()

    small = [
        pltpu.make_async_copy(src, vecs.at[i], v_sem.at[i])
        for i, src in enumerate((ag_h, as_h, cg_h, cs_h))
    ]
    weights = [
        pltpu.make_async_copy(src, dst, w_sem.at[i])
        for i, (src, dst) in enumerate(((wq_h, wq), (wk_h, wk), (wv_h, wv), (wo_h, wo)))
    ]
    taps = [
        pltpu.make_async_copy(
            wc_h.at[dy, dx], (wc.at[dx, 0], mid.at[dx], wc.at[dx, 3])[dy], wc_sem.at[3 * dy + dx]
        )
        for dy in range(3)
        for dx in range(3)
    ]

    def ring(way, blk, chunk, j):
        return pltpu.make_async_remote_copy(
            src_ref=kv.at[blk, chunk],
            dst_ref=kv.at[blk, chunk],
            send_sem=ring_send.at[way, j],
            recv_sem=ring_recv.at[way, j],
            device_id={"row": right if way == 0 else left},
        )

    def to_sib(blk, chunk, sends, recvs):
        return pltpu.make_async_remote_copy(
            src_ref=kv.at[blk, chunk],
            dst_ref=kv.at[blk, chunk],
            send_sem=sends,
            recv_sem=recvs,
            device_id={"row": sib},
        )

    def stat_copy(d, dst, sends, recvs):
        return pltpu.make_async_remote_copy(
            src_ref=mine,
            dst_ref=dst.at[d - 1],
            send_sem=sends.at[d - 1],
            recv_sem=recvs.at[d - 1],
            device_id={"row": (me + d) % DEV},
        )

    pl.semaphore_wait(barrier, 3)

    order = ((0, 2), (1, 3), (2, 0), (3, 1))
    loads[0].wait()
    ring(0, me, 0, 0).start()
    loads[2].wait()
    ring(1, me, 2, 0).start()
    loads[1].wait()
    loads[3].wait()
    for j in range(1, 3):
        ring(0, me, order[j][0], j).start()
        ring(1, me, order[j][1], j).start()

    for c in (*small, *weights):
        c.start()

    far_right = ((z + 2) % ZN) * 2 + core
    far_left = ((z + ZN - 2) % ZN) * 2 + core
    for k, peers in enumerate(((left, right, sib), (far_left, far_right), (sib,))):
        for peer in peers:
            pl.semaphore_signal(known.at[k], inc=1, device_id={"row": peer})
        if k == 0:
            base = kv[me, 0, 0:1, :].astype(F32)
            sums = [sums_about(base, kv[me, i].astype(F32)) for i in range(4)]
            put_moments(base, sum(a for a, _ in sums), sum(b for _, b in sums), mine)
        pl.semaphore_wait(known.at[k], len(peers))

    for d in range(1, DEV):
        stat_copy(d, stat_a, sa_send, sa_recv).start()
    for j in range(3, 4):
        ring(0, me, order[j][0], j).start()
        ring(1, me, order[j][1], j).start()
    for i in range(4):
        to_sib(me, i, own_send.at[i], own_recv.at[i]).start()

    m_s[...] = jnp.full_like(m_s, -1e30)
    l_s[...] = jnp.zeros_like(l_s)
    acc[...] = jnp.zeros_like(acc)

    for c in weights:
        c.wait()
    wv[...] = dot(wv[...], wo[...]).astype(BF16)

    def came(i):
        chunk = i % 4
        far = i // 4 + 1
        blk_r = ((z + ZN - far) % ZN) * 2 + core
        blk_l = ((z + far) % ZN) * 2 + core
        return blk_r, chunk, blk_l, (chunk + 2) % 4

    def comm(i):
        blk_r, cr, blk_l, cl = came(i)
        for way, blk, chunk in ((0, blk_r, cr), (1, blk_l, cl)):
            ring(way, blk, chunk, i).wait_recv()

            @pl.when(i < SENDS - 4)
            def _():
                ring(way, blk, chunk, i + 4).start()

            to_sib(blk, chunk, sib_send.at[way, i], sib_recv.at[way, i]).start()

    def attend(*chunks):
        keys = jnp.concatenate([kv[blk, chunk] for blk, chunk in chunks], axis=0)
        spans = range(0, CH * len(chunks), 128)

        def weigh(rows, s):
            m_old = m_s[rows, :]
            m_new = jnp.maximum(m_old, jnp.max(s, axis=1, keepdims=True))
            alpha = jnp.exp2(m_old - m_new)
            p = [jnp.exp2(s[:, k : k + 128] - m_new).astype(BF16) for k in spans]
            l_s[rows, :] = l_s[rows, :] * alpha + sum(v.astype(F32) for v in p)
            m_s[rows, :] = m_new
            return jnp.concatenate([alpha] * 4, axis=1), jnp.concatenate(p, axis=1)

        tiles = [pl.ds(TILE * t, TILE) for t in range(N // TILE)]
        s = dot(q_s[tiles[0], :], keys, NT)
        for t, rows in enumerate(tiles):
            ahead = dot(q_s[tiles[t + 1], :], keys, NT) if t + 1 < len(tiles) else None
            alpha, p = weigh(rows, s)
            acc[rows, :] = acc[rows, :] * alpha + dot(p, keys)
            s = ahead

    comm(0)

    for c in small:
        c.wait()
    for d in range(1, DEV):
        stat_copy(d, stat_a, sa_send, sa_recv).wait()
    comm(1)
    mean, rs = combined(stat_a, mine)
    scale = rs * vecs[0]
    shift = vecs[1]
    for i in range(4):
        normed = ((kv[me, i].astype(F32) - mean) * scale + shift).astype(BF16)
        query = dot(normed, wq[...]).astype(BF16)
        folded = dot(query, wk[...], NT) * (scale * (LOG2E / C**0.5))
        q_s[CH * i : CH * i + CH, :] = folded.astype(BF16)

    for i in range(4):
        to_sib(me, i, own_send.at[i], own_recv.at[i]).wait_recv()

    def first(k, carry):
        blk = jnp.where(k < 1, me, sib)
        attend((blk, 0), (blk, 1), (blk, 2), (blk, 3))
        return carry

    for c in taps:
        c.start()
    lax.fori_loop(0, 2, first, 0)

    def other(i):
        blk_r, cr, blk_l, cl = came(i)
        return blk_r + 1 - 2 * core, cr, blk_l + 1 - 2 * core, cl

    def sib_wait(i):
        blk_r, cr, blk_l, cl = other(i)
        to_sib(blk_r, cr, sib_send.at[0, i], sib_recv.at[0, i]).wait_recv()
        to_sib(blk_l, cl, sib_send.at[1, i], sib_recv.at[1, i]).wait_recv()

    def pair(blk_a, ca, blk_b, cb):
        return (blk_a, ca), (blk_b, cb)

    def spread_taps(k):
        dx, rows = k // 8, pl.ds(pl.multiple_of(k % 8 * 64, 64), 64)
        ends = (wc[dx, 0, rows, :].astype(F32) + wc[dx, 3, rows, :].astype(F32)) * -0.5
        half = mid[dx, rows, :].astype(F32) * -0.5
        wc[dx, 1, rows, :] = (ends + half).astype(BF16)
        wc[dx, 2, rows, :] = (ends - half).astype(BF16)

    for c in taps:
        c.wait()

    def body(i, carry):
        @pl.when(i < 13)
        def _():
            spread_taps(2 * i - 2)
            spread_taps(2 * i - 1)

        pl.when(i > 2)(lambda: comm(i))
        sib_wait(i - 1)
        attend(*pair(*other(i - 1)), *pair(*came(i)))
        return carry

    comm(2)
    attend(*pair(*came(0)))
    lax.fori_loop(1, SENDS, body, 0)
    def halo_copy(k, part):
        row, peer = ((ROWS - 1, (me + 1) % DEV), (0, (me + DEV - 1) % DEV))[k]
        piece = pl.ds(part * (W // 2), W // 2)
        return pltpu.make_async_remote_copy(
            src_ref=hid.at[row, piece],
            dst_ref=halo.at[k, piece],
            send_sem=h_send.at[k, part],
            recv_sem=h_recv.at[k, part],
            device_id={"row": peer},
        )

    sib_wait(SENDS - 1)
    keys = jnp.concatenate([kv[blk, chunk] for blk, chunk in pair(*other(SENDS - 1))], axis=0)
    tiles = ((0, 3), (1, 2))

    def of(ref, pair_rows):
        return jnp.concatenate([ref[W * r : W * r + W, :] for r in pair_rows], axis=0)

    total = jnp.zeros((8, C), F32)
    square = jnp.zeros((8, C), F32)
    s = dot(of(q_s, tiles[0]), keys, NT)
    for t, pair_rows in enumerate(tiles):
        ahead = dot(of(q_s, tiles[1]), keys, NT) if t == 0 else None
        m_old = of(m_s, pair_rows)
        m_new = jnp.maximum(m_old, jnp.max(s, axis=1, keepdims=True))
        alpha = jnp.exp2(m_old - m_new)
        p = [jnp.exp2(s[:, k : k + 128] - m_new).astype(BF16) for k in (0, 128)]
        den = of(l_s, pair_rows) * alpha + (p[0].astype(F32) + p[1].astype(F32))
        got = of(acc, pair_rows) * jnp.concatenate([alpha] * 4, axis=1)
        got = got + dot(jnp.concatenate(p, axis=1), keys)
        s = ahead
        inv = 1.0 / jnp.sum(den, axis=1, keepdims=True)
        att = ((got * inv - mean) * scale + shift).astype(BF16)
        x = jnp.concatenate([kv[me, r] for r in pair_rows], axis=0).astype(F32)
        h = (x + dot(att, wv[...])).astype(BF16)
        hid[pair_rows[0]] = h[:W]
        hid[pair_rows[1]] = h[W:]
        h = h.astype(F32)
        if pair_rows[0] == 0:
            base = h[0:1, :]
            for k in range(2):
                halo_copy(k, 0).start()
        a, b = sums_about(base, h)
        total = total + a
        square = square + b

    put_moments(base, total, square, mine)
    for d in range(1, DEV):
        stat_copy(d, stat_b, sb_send, sb_recv).start()
    for k in range(2):
        halo_copy(k, 1).start()
    def drain(i, carry):
        blk_r, cr, blk_l, cl = came(i)
        ring(0, blk_r, cr, i).wait_send()
        ring(1, blk_l, cl, i).wait_send()
        to_sib(blk_r, cr, sib_send.at[0, i], sib_recv.at[0, i]).wait_send()
        to_sib(blk_l, cl, sib_send.at[1, i], sib_recv.at[1, i]).wait_send()
        return carry

    lax.fori_loop(0, SENDS, drain, 0)
    for i in range(4):
        to_sib(me, i, own_send.at[i], own_recv.at[i]).wait_send()

    for k in range(2):
        for part in range(2):
            halo_copy(k, part).wait_send()
    for d in range(1, DEV):
        stat_copy(d, stat_b, sb_send, sb_recv).wait_send()
    for d in NEAREST:
        stat_copy(d, stat_b, sb_send, sb_recv).wait_recv()
    for k in range(2):
        for part in range(2):
            halo_copy(k, part).wait_recv()
    edges[...] = halo[...]
    mean2, rs2 = combined(stat_b, mine)
    coef[0] = mean2
    coef[1] = rs2 * vecs[2] * 0.5
    coef[2] = vecs[3] * 0.5


def conv_kernel(hid, edges, coef, wc, bias, out_hbm, mix_s, out_s, out_sem):
    me = lax.axis_index("row")
    mean, scale, shift = coef[0], coef[1], coef[2]

    for lo in range(0, W, FEW):
        d = []
        for j in range(ROWS + 2):
            src, r = (edges, 0) if j == 0 else (edges, 1) if j == ROWS + 1 else (hid, j - 1)
            half = (src[r, lo : lo + FEW, :].astype(F32) - mean) * scale + shift
            act = half + half * jnp.tanh(half)
            if j == 0:
                act = jnp.where(me == 0, 0.0, act)
            if j == ROWS + 1:
                act = jnp.where(me == DEV - 1, 0.0, act)
            d.append(act.astype(BF16))
        for a in range(2):
            e = d[2 * a : 2 * a + 4]
            for k, v in ((1, e[1] + e[2]), (2, e[2] - e[1]), (0, e[0] - e[2]), (3, e[1] - e[3])):
                mix_s[k, W * a + lo : W * a + lo + FEW, :] = v

    part = C // SPLIT
    col = lax.broadcasted_iota(jnp.int32, (2 * W, part), 0) % W
    copies = []
    for n in range(SPLIT):
        cols = slice(part * n, part * n + part)
        rows = [None, None]
        for dx in (1, 0, 2):
            m = [None] * 4
            for k in (1, 2, 0, 3):
                m[k] = dot(mix_s[k], wc[dx, k, :, cols])
            for i, v in enumerate((m[0] - m[1] - m[2], m[2] - m[1] - m[3])):
                if dx == 0:
                    v = jnp.where(col == 0, 0.0, pltpu.roll(v, 1, 0))
                if dx == 2:
                    v = jnp.where(col == W - 1, 0.0, pltpu.roll(v, 2 * W - 1, 0))
                rows[i] = v if rows[i] is None else rows[i] + v
        for r in range(ROWS):
            total = rows[r % 2][W * (r // 2) : W * (r // 2) + W]
            base = hid[r, :, cols].astype(F32)
            out_s[W * r : W * r + W, cols] = (base + (total + bias[:, cols])).astype(BF16)
        copies.append(
            pltpu.make_async_copy(out_s.at[:, cols], out_hbm.at[:, cols], out_sem.at[n])
        )
        copies[-1].start()
    for c in copies:
        c.wait()


def local(
    latent, attn_gain, attn_shift, w_query, w_key, w_value, w_out,
    conv_gain, conv_shift, w_conv, conv_bias,
):
    line = lambda v: v.reshape(1, C)
    dma = pltpu.SemaphoreType.DMA
    vmem = pl.BlockSpec(memory_space=pltpu.VMEM)
    hid, edges, coef, taps = pl.pallas_call(
        kernel,
        out_shape=(
            pltpu.VMEM((ROWS, W, C), BF16),
            pltpu.VMEM((2, W, C), BF16),
            pltpu.VMEM((3, 1, C), F32),
            pltpu.VMEM((3, 4, C, C), BF16),
        ),
        in_specs=[pl.BlockSpec(memory_space=pltpu.HBM)] * 10,
        out_specs=(vmem,) * 4,
        scratch_shapes=[
            pltpu.VMEM((DEV, 4, CH, C), BF16),
            pltpu.VMEM((C, C), BF16),
            pltpu.VMEM((C, C), BF16),
            pltpu.VMEM((C, C), BF16),
            pltpu.VMEM((C, C), BF16),
            pltpu.VMEM((3, C, C), BF16),
            pltpu.VMEM((4, 1, C), F32),
            pltpu.VMEM((N, C), BF16),
            pltpu.VMEM((N, C), F32),
            pltpu.VMEM((N, 128), F32),
            pltpu.VMEM((N, 128), F32),
            pltpu.VMEM((2, W, C), BF16),
            pltpu.VMEM((1, 128), F32),
            pltpu.VMEM((DEV - 1, 1, 128), F32),
            pltpu.VMEM((DEV - 1, 1, 128), F32),
            dma((4,)),
            dma((4,)),
            dma((9,)),
            dma((4,)),
            dma((2, SENDS)),
            dma((2, SENDS)),
            dma((2, SENDS)),
            dma((2, SENDS)),
            dma((4,)),
            dma((4,)),
            dma((DEV - 1,)),
            dma((DEV - 1,)),
            dma((DEV - 1,)),
            dma((DEV - 1,)),
            dma((2, 2)),
            dma((2, 2)),
            pltpu.SemaphoreType.REGULAR((3,)),
        ],
        compiler_params=pltpu.CompilerParams(
            collective_id=0, has_side_effects=True, vmem_limit_bytes=30 * 1024 * 1024
        ),
    )(
        *(
            pltpu.with_memory_space_constraint(v, pltpu.HBM)
            for v in (
                latent.reshape(N, C), line(attn_gain), line(attn_shift), w_query, w_key,
                w_value, w_out, line(conv_gain), line(conv_shift), w_conv,
            )
        )
    )
    out = pl.pallas_call(
        conv_kernel,
        out_shape=jax.ShapeDtypeStruct((N, C), BF16),
        in_specs=[vmem] * 5,
        out_specs=pl.BlockSpec(memory_space=pltpu.HBM),
        scratch_shapes=[
            pltpu.VMEM((4, 2 * W, C), BF16),
            pltpu.VMEM((N, C), BF16),
            dma((SPLIT,)),
        ],
        compiler_params=pltpu.CompilerParams(vmem_limit_bytes=28 * 1024 * 1024),
    )(hid, edges, coef, taps, line(conv_bias))
    return out.reshape(ROWS, W, C)


def solution(mesh):
    part = P(("img", "row"), None, None)
    return jax.shard_map(
        local, mesh=mesh, in_specs=(part,) + (P(),) * 10, out_specs=part, check_vma=False
    )
```
